256 devices in a mesh: dp: 256 (over y, z, x, core).
Axes of the slice: x: 4, y: 4, z: 8, core: 2. Of those that a mesh axis runs over, the one named last changes fastest.
Arguments:
- master: float32 [524288], P('dp'), may hold values from -6 to 6
- gradients: float32 [524288], P('dp'), may hold values from -6 to 6
- first_moment: float32 [524288], P('dp'), may hold values from -4 to 4
- second_moment: float32 [524288], P('dp'), may hold values from 0.01 to 1
- segment_ids: int32 [524288], P('dp'), may hold values from 0 to 511, as said below
- decay_mask: int32 [512], replicated, may hold values 0 or 1
Outputs:
- new_master: float32 [524288], P('dp')
- new_first: float32 [524288], P('dp')
- new_second: float32 [524288], P('dp')
- scaled_step: float32 [524288], P('dp')
- model_weights: bfloat16 [524288], replicated
The draws below stay inside these ranges and needn't reach their ends.
Inputs may be any that keep to these rules, and one draw needn't show every extreme that they name: segment_ids never falls along the flat vector; each tensor 0 to 511 owns one contiguous run of 256 to 16384 elements, and one tensor has exactly 16384. `decay_mask`: each entry is 0 or 1.
All inputs are finite; a program needn't handle non-finite values.
Results may differ from the reference program's by a relative error of at most 0.0004.
Values may be sent and summed in bfloat16 or wider, within the bound.
A program may use at most 64 MiB of HBM per device.

```python
import math
import jax
import jax.numpy as jnp

P_DEV = 2048
SEG_DEV = 2
STEP = 20
PARAMS = 524288
TENSORS = 512


def draw_segment_ids(key, part):
    weight_key = jax.random.fold_in(key, 11)
    place_key = jax.random.fold_in(key, 23)
    shortest = P_DEV // (4 * SEG_DEV)
    longest = 8 * P_DEV
    shares = jax.random.randint(weight_key, (TENSORS - 1,), 1, 8).astype(jnp.int32)
    remain = PARAMS - longest - (TENSORS - 1) * shortest
    total = jnp.sum(shares)
    running = jnp.cumsum(shares)
    bounds = remain // total * running + remain % total * running // total
    extra = jnp.diff(jnp.concatenate([jnp.zeros((1,), jnp.int32), bounds.astype(jnp.int32)]))
    others = shortest + extra
    place = jax.random.randint(place_key, (), 0, TENSORS).astype(jnp.int32)
    tensor_index = jnp.arange(TENSORS, dtype=jnp.int32)
    source = jnp.clip(tensor_index - (tensor_index > place).astype(jnp.int32), 0, TENSORS - 2)
    lengths = jnp.where(tensor_index == place, longest, others[source]).astype(jnp.int32)
    finish = jnp.cumsum(lengths)
    positions = jnp.arange(PARAMS, dtype=jnp.int32)
    return jnp.searchsorted(finish, positions, side='right').astype(jnp.int32)


def set_ends(entries, own_key, low, largest):
    spot = [jax.random.randint(jax.random.fold_in(own_key, axis), (), 0, length) for axis, length in enumerate(entries.shape)]
    widest = entries.shape.index(max(entries.shape))
    next_to = spot[:widest] + [(spot[widest] + 1) % entries.shape[widest]] + spot[widest + 1:]
    return entries.at[tuple(spot)].set(low).at[tuple(next_to)].set(largest)


def levels(own_key, shape, pieces, least, high):
    def one(position, parts):
        heights = jax.random.uniform(jax.random.fold_in(jax.random.fold_in(own_key, 6), position), (parts,), jnp.float32, least / len(pieces), high / len(pieces))
        return jnp.repeat(jnp.exp(heights), shape[position] // parts).reshape((-1,) + (1,) * (len(shape) - position - 1))

    loudness = one(*pieces[0])
    for cut in pieces[1:]:
        loudness = loudness * one(*cut)
    return loudness


def normal_values(own_key, shape, scale, reach, split=(), held_as=jnp.bfloat16):
    array = jax.random.normal(own_key, shape, jnp.float32) * scale
    if len(split) > 0:
        array = levels(own_key, shape, split, -0.22, 0.18) * array
    return jnp.clip(array, min=-reach, max=reach).astype(held_as)


def setup_inputs(seed: int = 0) -> dict:
    streams_of = jax.random.split(jax.random.key(seed), 7)
    master = normal_values(streams_of[0], (PARAMS,), 1.0, 6.0, ((0, 256),), jnp.float32)
    gradients = normal_values(streams_of[1], (PARAMS,), 1.0, 6.0, ((0, 256),), jnp.float32)
    first_moment = normal_values(streams_of[2], (PARAMS,), 0.3, 4.0, ((0, 256),), jnp.float32)
    second_moment = jnp.clip(jnp.exp(math.log(1.0) - 4.6051702 * jax.random.uniform(streams_of[3], (PARAMS,), jnp.float32) ** levels(streams_of[3], (PARAMS,), ((0, 256),), -0.2, 0.2)), 0.01, 1.0)
    segment_ids = draw_segment_ids(jax.random.fold_in(streams_of[6], 71), 0)
    decay_mask = set_ends((jax.random.randint(streams_of[5], (TENSORS,), 0, 2) < 1).astype(jnp.int32), jax.random.fold_in(streams_of[5], 1), 0, 1)
    return {"master": master, "gradients": gradients, "first_moment": first_moment, "second_moment": second_moment, "segment_ids": segment_ids, "decay_mask": decay_mask}


first_decay = 0.9
second_decay = 0.999
epsilon = 1e-06
weight_decay = 0.01
learn_rate = 0.006

def adam_direction(master, gradients, first_moment, second_moment, decay):
    new_first = first_decay * first_moment + (1.0 - first_decay) * gradients
    new_second = second_decay * second_moment + (1.0 - second_decay) * gradients * gradients
    hat_first = new_first / (1.0 - first_decay ** STEP)
    hat_second = new_second / (1.0 - second_decay ** STEP)
    direction = hat_first / (jnp.sqrt(hat_second) + epsilon) + weight_decay * decay * master
    return (new_first, new_second, direction)

def trust_ratio(weight_sq, step_sq):
    weight_norm = jnp.sqrt(weight_sq)
    step_norm = jnp.sqrt(step_sq)
    usable = (weight_norm > 0.0) & (step_norm > 0.0)
    return jnp.where(usable, weight_norm / jnp.where(usable, step_norm, 1.0), 1.0)

def reference(master, gradients, first_moment, second_moment, segment_ids, decay_mask):
    decay = decay_mask.astype(jnp.float32)[segment_ids]
    new_first, new_second, direction = adam_direction(master, gradients, first_moment, second_moment, decay)
    weight_sq = jax.ops.segment_sum(master * master, segment_ids, num_segments=TENSORS)
    step_sq = jax.ops.segment_sum(direction * direction, segment_ids, num_segments=TENSORS)
    scaled_step = trust_ratio(weight_sq, step_sq)[segment_ids] * direction
    new_master = master - learn_rate * scaled_step
    return (new_master, new_first, new_second, scaled_step, new_master.astype(jnp.bfloat16))
```

```python
import functools

import jax
import jax.numpy as jnp
from jax import lax
from jax.experimental import pallas as pl
from jax.experimental.pallas import tpu as pltpu
from jax.sharding import PartitionSpec as P

STEP = 20
first_decay = 0.9
second_decay = 0.999
epsilon = 1e-06
weight_decay = 0.01
learn_rate = 0.006

NY, NZ, NX, NC = 4, 8, 4, 2
DEVICES = NY * NZ * NX * NC
ROWS, LANES = 16, 128
REACH = 8
SEGMENTS = 9
MESH = pl.DeviceIdType.MESH


def adam_direction(master, gradients, first_moment, second_moment, decay):
    new_first = first_decay * first_moment + (1.0 - first_decay) * gradients
    new_second = second_decay * second_moment + (1.0 - second_decay) * gradients * gradients
    hat_first = new_first / (1.0 - first_decay**STEP)
    hat_second = new_second / (1.0 - second_decay**STEP)
    direction = hat_first / (jnp.sqrt(hat_second) + epsilon) + weight_decay * decay * master
    return (new_first, new_second, direction)


def trust_ratio(weight_sq, step_sq):
    weight_norm = jnp.sqrt(weight_sq)
    step_norm = jnp.sqrt(step_sq)
    usable = (weight_norm > 0.0) & (step_norm > 0.0)
    return jnp.where(usable, weight_norm / jnp.where(usable, step_norm, 1.0), 1.0)


def total_of(values):
    return jnp.sum(jnp.sum(values, axis=0, keepdims=True), axis=1, keepdims=True)


def kernel(
    master_hbm, grad_hbm, first_hbm, second_hbm, ids_hbm, mask_hbm,
    new_master_ref, new_first_ref, new_second_ref, scaled_ref, gathered,
    master_ref, grad_ref, first_ref, second_ref, ids_ref, ids_smem, mask_smem,
    outgoing, incoming,
    in_sems, stat_send, stat_recv, z_send, z_recv, p_send, p_recv, q_send, q_recv, d_send, d_recv,
):
    me = lax.axis_index("dp")
    c = lax.rem(me, 2)
    x = lax.rem(me // 2, NX)
    z = lax.rem(me // 8, NZ)
    y = me // 64

    def device(yy, zz, xx, cc):
        return ((yy * NZ + zz) * NX + xx) * NC + cc

    def shifted(offset):
        return lax.rem(me + offset + DEVICES, DEVICES)

    class_a = 1 - c

    def p_peer(k):
        return device(
            lax.rem(y + class_a * k, NY), z, lax.rem(x + c * k, NX), c
        )

    def q_peer(k):
        return device(
            lax.rem(y + c * k, NY), z, lax.rem(x + class_a * k, NX), c
        )

    def column(core, pj, qk):
        a = 1 - core
        yy = lax.rem(y + a * pj + core * qk, NY)
        xx = lax.rem(x + core * pj + a * qk, NX)
        return gathered.at[yy, :, xx, core]

    z_peers = [device(y, lax.rem(z + k, NZ), x, c) for k in range(1, NZ)]
    p_peers = [p_peer(k) for k in range(1, 4)]
    q_peers = [q_peer(k) for k in range(1, 4)]
    sibling = device(y, z, x, 1 - c)
    up = [shifted(k) for k in range(1, REACH + 1)]
    down = [shifted(-k) for k in range(1, REACH + 1)]

    barrier = pltpu.get_barrier_semaphore()
    partners = up + down + z_peers + p_peers + q_peers + [sibling]
    for partner in partners:
        pl.semaphore_signal(barrier, inc=1, device_id=(partner,), device_id_type=MESH)

    loads = [
        pltpu.make_async_copy(src, dst, in_sems.at[i])
        for i, (src, dst) in enumerate(
            [
                (ids_hbm, ids_smem),
                (mask_hbm, mask_smem),
                (ids_hbm, ids_ref),
                (master_hbm, master_ref),
                (grad_hbm, grad_ref),
                (first_hbm, first_ref),
                (second_hbm, second_ref),
            ]
        )
    ]
    for load in loads:
        load.start()
    for load in loads:
        load.wait()

    first_id = ids_smem[0, 0]
    last_id = ids_smem[ROWS - 1, LANES - 1]
    last_local = last_id - first_id
    local = ids_ref[...] - first_id
    decay = jnp.zeros((ROWS, LANES), jnp.float32)
    for k in range(SEGMENTS):
        value = mask_smem[jnp.minimum(first_id + k, mask_smem.shape[0] - 1)]
        decay = jnp.where(local == k, value.astype(jnp.float32), decay)

    master = master_ref[...]
    new_first, new_second, direction = adam_direction(
        master, grad_ref[...], first_ref[...], second_ref[...], decay
    )
    new_first_ref[...] = new_first
    new_second_ref[...] = new_second
    weight_square = master * master
    step_square = direction * direction

    def masked(index):
        hit = local == index
        return (
            total_of(jnp.where(hit, weight_square, 0.0)),
            total_of(jnp.where(hit, step_square, 0.0)),
        )

    head_w, head_s = masked(0)
    tail_w, tail_s = masked(last_local)
    shape = (1, LANES)
    for slot, (key, w, s) in enumerate(
        [(last_id, tail_w, tail_s), (first_id, head_w, head_s)]
    ):
        outgoing[slot, 0:1, :] = jnp.full(shape, key.astype(jnp.float32))
        outgoing[slot, 1:2, :] = jnp.broadcast_to(w, shape)
        outgoing[slot, 2:3, :] = jnp.broadcast_to(s, shape)

    pl.semaphore_wait(barrier, len(partners))

    stats = []
    for k in range(REACH):
        for way, peers in ((0, up), (1, down)):
            slot = way * REACH + k
            copy = pltpu.make_async_remote_copy(
                src_ref=outgoing.at[way],
                dst_ref=incoming.at[slot],
                send_sem=stat_send.at[slot],
                recv_sem=stat_recv.at[slot],
                device_id=(peers[k],),
                device_id_type=MESH,
            )
            copy.start()
            stats.append(copy)

    trust = jnp.ones((ROWS, LANES), jnp.float32)
    for k in range(1, SEGMENTS - 1):
        w, s = masked(k)
        trust = jnp.where(local == k, trust_ratio(w, s), trust)

    for copy in stats:
        copy.wait_recv()
    sums = [jnp.broadcast_to(v, shape) for v in (head_w, head_s, tail_w, tail_s)]
    for key, base in ((first_id, 0), (last_id, 2)):
        target = key.astype(jnp.float32)
        for slot in range(2 * REACH):
            hit = incoming[slot, 0:1, :] == target
            sums[base] += jnp.where(hit, incoming[slot, 1:2, :], 0.0)
            sums[base + 1] += jnp.where(hit, incoming[slot, 2:3, :], 0.0)
    trust = jnp.where(local == last_local, trust_ratio(sums[2], sums[3]), trust)
    trust = jnp.where(local == 0, trust_ratio(sums[0], sums[1]), trust)

    scaled = trust * direction
    new_master = master - learn_rate * scaled
    gathered[y, z, x, c] = new_master.astype(jnp.bfloat16)

    def send(block, send_sem, recv_sem, peer):
        copy = pltpu.make_async_remote_copy(
            src_ref=block,
            dst_ref=block,
            send_sem=send_sem,
            recv_sem=recv_sem,
            device_id=(peer,),
            device_id_type=MESH,
        )
        copy.start()
        return copy

    def arrived(block, send_sem, recv_sem):
        pltpu.make_async_remote_copy(
            src_ref=block,
            dst_ref=block,
            send_sem=send_sem,
            recv_sem=recv_sem,
            device_id=(me,),
            device_id_type=MESH,
        ).wait_recv()

    sends = []
    own = gathered.at[y, z, x, c]
    for k in (4, 3, 5, 2, 6, 1, 7):
        sends.append(send(own, z_send.at[k - 1], z_recv.at[k - 1], z_peers[k - 1]))
    new_master_ref[...] = new_master
    scaled_ref[...] = scaled
    for k in (7, 1, 6, 2, 5, 3, 4):
        arrived(
            gathered.at[y, lax.rem(z + NZ - k, NZ), x, c], z_send.at[k - 1], z_recv.at[k - 1]
        )

    mine = column(c, 0, 0)
    for k in (2, 1, 3):
        sends.append(send(mine, p_send.at[k - 1], p_recv.at[k - 1], p_peers[k - 1]))

    def spread_block(j):
        block = column(c, j, 0)
        for k in (2, 1, 3):
            slot = j * 3 + k - 1
            sends.append(send(block, q_send.at[slot], q_recv.at[slot], q_peers[k - 1]))
        sends.append(send(block, d_send.at[j * 4], d_recv.at[j * 4], sibling))

    spread_block(0)
    for k in (1, 3, 2):
        j = 4 - k
        arrived(column(c, j, 0), p_send.at[k - 1], p_recv.at[k - 1])
        spread_block(j)
    for j in (0, 3, 1, 2):
        for k in (1, 3, 2):
            slot = j * 3 + k - 1
            block = column(c, j, 4 - k)
            arrived(block, q_send.at[slot], q_recv.at[slot])
            label = j * 4 + 4 - k
            sends.append(send(block, d_send.at[label], d_recv.at[label], sibling))
    for j in range(4):
        for k in range(4):
            label = j * 4 + k
            arrived(column(1 - c, j, k), d_send.at[label], d_recv.at[label])
    for copy in stats:
        copy.wait_send()
    for copy in sends:
        copy.wait_send()


def shards(master, gradients, first_moment, second_moment, segment_ids, decay_mask):
    tile = (ROWS, LANES)
    f32 = jax.ShapeDtypeStruct(tile, jnp.float32)
    dma = pltpu.SemaphoreType.DMA
    outs = pl.pallas_call(
        kernel,
        out_shape=[f32, f32, f32, f32,
                   jax.ShapeDtypeStruct((NY, NZ, NX, NC, ROWS, LANES), jnp.bfloat16)],
        in_specs=[pl.BlockSpec(memory_space=pl.ANY)] * 6,
        out_specs=[pl.BlockSpec(memory_space=pltpu.VMEM)] * 5,
        scratch_shapes=[
            pltpu.VMEM(tile, jnp.float32),
            pltpu.VMEM(tile, jnp.float32),
            pltpu.VMEM(tile, jnp.float32),
            pltpu.VMEM(tile, jnp.float32),
            pltpu.VMEM(tile, jnp.int32),
            pltpu.SMEM(tile, jnp.int32),
            pltpu.SMEM((512,), jnp.int32),
            pltpu.VMEM((2, 4, LANES), jnp.float32),
            pltpu.VMEM((2 * REACH, 4, LANES), jnp.float32),
            dma((7,)), dma((16,)), dma((16,)), dma((7,)), dma((7,)),
            dma((3,)), dma((3,)), dma((12,)), dma((12,)), dma((16,)), dma((16,)),
        ],
        compiler_params=pltpu.CompilerParams(collective_id=0, has_side_effects=True),
        name="lamb",
    )(
        master.reshape(tile), gradients.reshape(tile), first_moment.reshape(tile),
        second_moment.reshape(tile), segment_ids.reshape(tile), decay_mask,
    )
    new_master, new_first, new_second, scaled, weights = outs
    return (
        new_master.reshape(-1), new_first.reshape(-1), new_second.reshape(-1),
        scaled.reshape(-1), weights.reshape(-1),
    )


def solution(mesh):
    return jax.shard_map(
        shards,
        mesh=mesh,
        in_specs=(P("dp"), P("dp"), P("dp"), P("dp"), P("dp"), P()),
        out_specs=(P("dp"), P("dp"), P("dp"), P("dp"), P()),
        check_vma=False,
    )
```
